512 devices in a mesh: grp: 2 (over y), ctx: 32 (over z, core), hd: 8 (over x).
Axes of the slice: x: 8, y: 2, z: 16, core: 2. Of those that a mesh axis runs over, the one named last changes fastest.
The devices are a block of a 8x8x16 slice.
Arguments:
- query: bfloat16 [8192, 4096], P(('grp', 'ctx'), 'hd'), parts along dimension 0, may hold values from -6 to 6
- keys: bfloat16 [8192, 1024], P(('grp', 'ctx'), 'hd'), parts along dimension 0, may hold values from -6 to 6
- values: bfloat16 [8192, 1024], P(('grp', 'ctx'), 'hd'), parts along dimension 0, may hold values from -6 to 6
- m_x: bfloat16 [8192, 8192], P(('grp', 'ctx'), 'hd'), parts along dimension 0, may hold values from -6 to 6
- m_z: bfloat16 [8192, 8192], P(('grp', 'ctx'), 'hd'), parts along dimension 0, may hold values from -6 to 6
- m_b: bfloat16 [8192, 1024], P(('grp', 'ctx'), 'hd'), parts along dimension 0, may hold values from -6 to 6
- m_c: bfloat16 [8192, 1024], P(('grp', 'ctx'), 'hd'), parts along dimension 0, may hold values from -0.5 to 0.5
- dt_raw: bfloat16 [8192, 128], P(('grp', 'ctx'), 'hd'), parts along dimension 0, may hold values from -5 to 204
- dt_bias: float32 [128], P('hd'), may hold values from -0.5 to 0.5
- a_log: float32 [128], P('hd'), may hold values from -10 to 0
- d_skip: float32 [128], P('hd'), may hold values from 0.5 to 2
- norm_gain: float32 [8192], P('hd'), may hold values from 0.5 to 1.5
Outputs:
- context: bfloat16 [8192, 4096], P(('grp', 'ctx'), 'hd'), parts along dimension 0
- mixed: bfloat16 [8192, 8192], P(('grp', 'ctx'), 'hd'), parts along dimension 0
The draws below stay inside these ranges and needn't reach their ends.
There are 2 independent parts, one for each index of `grp`. The reference program is written for one: setup_inputs(seed, part) draws one part's arguments, and reference() takes and returns one part's arrays. A program takes and returns all parts, laid end to end along the dimension named above; an argument that names none is the same for every part. Nothing has to cross between parts.
All inputs are finite; a program needn't handle non-finite values.
Results may differ from the reference program's by a relative error of at most 0.009.
Values may be sent and summed in bfloat16 or wider, within the bound.
No kernel may reach another device: no remote copies, remote signals or barrier semaphores. Data moves between devices by JAX's collectives and lax.ppermute only.
A program may use at most 64 MiB of HBM per device.

```python
import math
import jax
import jax.numpy as jnp
from jax import lax

QUERY_HEADS = 32
KEY_VALUE_HEADS = 8
HEAD_SIZE = 128
MH = 128
MP = 64
MN = 128
MG = 8
TOK_DEV = 128
SEQUENCE_TOKENS = 4096
N_CTX = 32


def spike_rows(key):
    return jax.random.randint(jax.random.fold_in(key, 101), (2,), 0, SEQUENCE_TOKENS)


def spike_level():
    return min(SEQUENCE_TOKENS // 20, 256)


def draw_keys(key, part):
    random_seed_key = jax.random.fold_in(key, 606)
    sampled = jnp.clip(jax.random.normal(random_seed_key, (SEQUENCE_TOKENS, KEY_VALUE_HEADS * HEAD_SIZE), jnp.float32), -6.0, 6.0)
    return sampled.astype(jnp.bfloat16)


def draw_query(key, part):
    random_seed_key = jax.random.fold_in(key, 707)
    sampled = jnp.clip(jax.random.normal(random_seed_key, (SEQUENCE_TOKENS, QUERY_HEADS * HEAD_SIZE), jnp.float32), -6.0, 6.0)
    return sampled.astype(jnp.bfloat16)


def draw_m_x(key, part):
    selected = spike_rows(key)
    first_key = jax.random.fold_in(jax.random.fold_in(key, 303), 0)
    sampled = jax.random.normal(first_key, (SEQUENCE_TOKENS, MH * MP), jnp.float32)
    sampled = jnp.clip(sampled, -6.0, 6.0)
    flagged = jnp.any(jnp.arange(SEQUENCE_TOKENS)[:, None] == selected[None, :], axis=1)
    sampled = jnp.where(flagged[:, None], sampled * (0.06 / spike_level()), sampled)
    return sampled.astype(jnp.bfloat16)


def draw_dt_raw(key, part):
    selected = spike_rows(key)
    first_key, other_random_key = jax.random.split(jax.random.fold_in(key, 202))
    rough = jax.random.uniform(first_key, (SEQUENCE_TOKENS, MH), jnp.float32, -1.0, 1.0) - 3.0
    offsets = jax.random.uniform(other_random_key, (SEQUENCE_TOKENS // TOK_DEV, 1), jnp.float32, -0.7, 0.7)
    sampled = rough + jnp.repeat(offsets, TOK_DEV, axis=0)
    flagged = jnp.any(jnp.arange(SEQUENCE_TOKENS)[:, None] == selected[None, :], axis=1)
    sampled = jnp.where(flagged[:, None], jnp.float32(spike_level()), sampled)
    return sampled.astype(jnp.bfloat16)


def draw_a_log(key, part):
    first_key, other_random_key, third_key = jax.random.split(jax.random.fold_in(key, 404), 3)
    quick = jax.random.bernoulli(first_key, 0.5, (MH,))
    window = jax.random.uniform(other_random_key, (MH,), jnp.float32, 20.0, 60.0)
    slack = jax.random.uniform(third_key, (MH,), jnp.float32, 0.3, 1.0)
    fast_rate = -jnp.log(0.06 * window)
    slow_rate = -jnp.log(0.06 * SEQUENCE_TOKENS) - slack
    return jnp.where(quick, fast_rate, slow_rate).astype(jnp.float32)


def block_levels(rng, shape, cuts, least, top_value):
    level = 1.0
    for position, blocks in cuts:
        steps = jax.random.uniform(jax.random.fold_in(jax.random.fold_in(rng, 6), position), (blocks,), jnp.float32, least / len(cuts), top_value / len(cuts))
        level = level * jnp.repeat(jnp.exp(steps), shape[position] // blocks).reshape((-1,) + (1,) * (len(shape) - 1 - position))
    return level


def noise(own_key, extent, scale, bound, shards=(), kind=jnp.bfloat16):
    level = block_levels(own_key, extent, shards, -0.22, 0.18) if shards else 1.0
    values = jax.random.normal(own_key, extent, jnp.float32) * scale * level
    return jnp.minimum(jnp.maximum(values, -bound), bound).astype(kind)


def setup_inputs(seed: int = 0, part: int = 0) -> dict:
    streams_of = jax.random.split(jax.random.key(seed), 13)
    part_keys = jax.random.split(jax.random.fold_in(streams_of[12], part), 13)
    return {
        "query": draw_query(jax.random.fold_in(jax.random.fold_in(streams_of[12], part), 71), part),
        "keys": draw_keys(jax.random.fold_in(jax.random.fold_in(streams_of[12], part), 71), part),
        "values": noise(part_keys[2], (SEQUENCE_TOKENS, KEY_VALUE_HEADS * HEAD_SIZE), 1.0, 6.0, ((0, 32), (1, 8))),
        "m_x": draw_m_x(jax.random.fold_in(jax.random.fold_in(streams_of[12], part), 71), part),
        "m_z": noise(part_keys[4], (SEQUENCE_TOKENS, MH * MP), 1.0, 6.0, ((0, 32), (1, 8))),
        "m_b": noise(part_keys[5], (SEQUENCE_TOKENS, MG * MN), 1.0, 6.0, ((0, 32), (1, 8))),
        "m_c": noise(part_keys[6], (SEQUENCE_TOKENS, MG * MN), MN ** -0.5, 0.5, ((0, 32), (1, 8))),
        "dt_raw": draw_dt_raw(jax.random.fold_in(jax.random.fold_in(streams_of[12], part), 71), part),
        "dt_bias": jnp.clip(jax.random.uniform(streams_of[8], (MH,), jnp.float32, -0.5, 0.5) * block_levels(streams_of[8], (MH,), ((0, 8),), -0.4, 0.0), -0.5, 0.5),
        "a_log": draw_a_log(jax.random.fold_in(streams_of[12], 71), part),
        "d_skip": jnp.clip(0.5 + 1.5 * jax.random.uniform(streams_of[10], (MH,), jnp.float32) ** block_levels(streams_of[10], (MH,), ((0, 8),), -0.2, 0.2), 0.5, 2.0),
        "norm_gain": jnp.clip(1.0 + 0.1 * jax.random.normal(streams_of[11], (MH * MP,), jnp.float32), 0.5, 1.5),
    }


highest = lax.Precision.HIGHEST
norm_eps = 1e-05

def folded_to_sequence(whole):
    half_rows = whole.shape[0] // (2 * N_CTX)
    blocks = whole.reshape((N_CTX, 2, half_rows) + whole.shape[1:])
    return jnp.concatenate([blocks[:, 0], blocks[::-1, 1]], axis=0).reshape(whole.shape)

def attention(query, keys, values):
    sequence_length = query.shape[0]
    heads_per_group = QUERY_HEADS // KEY_VALUE_HEADS
    every_query = query.astype(jnp.float32).reshape(sequence_length, KEY_VALUE_HEADS, heads_per_group, HEAD_SIZE)
    every_key = keys.astype(jnp.float32).reshape(sequence_length, KEY_VALUE_HEADS, HEAD_SIZE)
    every_value = values.astype(jnp.float32).reshape(sequence_length, KEY_VALUE_HEADS, HEAD_SIZE)
    rows_per_block = math.gcd(sequence_length, 256)
    query_block_list = every_query.reshape(sequence_length // rows_per_block, rows_per_block, KEY_VALUE_HEADS, heads_per_group, HEAD_SIZE)
    key_pos = jnp.arange(sequence_length, dtype=jnp.int32)

    def query_block(packed):
        block_query, block_index = packed
        query_pos = block_index * rows_per_block + jnp.arange(rows_per_block, dtype=jnp.int32)
        scores = jnp.einsum('qhgd,khd->hgqk', block_query, every_key, precision=highest) / math.sqrt(HEAD_SIZE)
        visible = key_pos[None, :] <= query_pos[:, None]
        scores = jnp.where(visible, scores, -jnp.inf)
        largest = lax.optimization_barrier(jnp.max(scores, axis=-1, keepdims=True))
        expons = jnp.exp(scores - largest)
        totals = lax.optimization_barrier(jnp.sum(expons, axis=-1))
        rounded = lax.optimization_barrier(expons.astype(jnp.bfloat16)).astype(jnp.float32)
        summed = jnp.einsum('hgqk,khd->qhgd', rounded, every_value, precision=highest)
        return (summed / jnp.transpose(totals, (2, 0, 1))[..., None]).reshape(rows_per_block, QUERY_HEADS * HEAD_SIZE)
    result = lax.map(query_block, (query_block_list, jnp.arange(sequence_length // rows_per_block, dtype=jnp.int32)))
    return result.reshape(sequence_length, QUERY_HEADS * HEAD_SIZE).astype(jnp.bfloat16)

def ssd_block(inputs, steps, rates, b_rows, c_rows):
    intersection = jnp.dot(c_rows, b_rows.T, preferred_element_type=jnp.float32)
    inputs = inputs.astype(jnp.float32)
    b_rows = b_rows.astype(jnp.float32)
    sequence_length = inputs.shape[0]
    running = jnp.cumsum(-steps * rates, axis=0)
    lower = jnp.arange(sequence_length)[:, None] >= jnp.arange(sequence_length)[None, :]
    spread = running[:, None, :] - running[None, :, :]
    decay = jnp.exp(jnp.where(lower[:, :, None], spread, -jnp.inf))
    weights = intersection[:, :, None] * decay * steps[None, :, :]
    inner = jnp.einsum('ijh,jhp->ihp', weights, inputs, precision=highest)
    tail_weight = jnp.exp(running[-1][None, :] - running) * steps
    state = jnp.einsum('jh,jhp,jn->hpn', tail_weight, inputs, b_rows, precision=highest)
    return (inner, state, jnp.exp(running[-1]), jnp.exp(running))

def chain_states(earlier, later):
    return (earlier[0] * later[0], earlier[1] * later[0][..., None, None] + later[1])

def ssd_sequence(inputs, steps, rates, b_rows, c_rows):
    sequence_length, head_count, width = inputs.shape
    block_len = math.gcd(sequence_length, 128)
    count = sequence_length // block_len
    c_blocks = c_rows.reshape(count, block_len, -1)
    inner, state, totals, scaled = jax.vmap(ssd_block, in_axes=(0, 0, None, 0, 0))(inputs.reshape(count, block_len, head_count, width), steps.reshape(count, block_len, head_count), rates, b_rows.reshape(count, block_len, -1), c_blocks)
    running = lax.associative_scan(chain_states, (totals, state))
    entering = jnp.concatenate([jnp.zeros_like(running[1][:1]), running[1][:-1]], axis=0)
    carried = jnp.einsum('cqn,chpn->cqhp', c_blocks.astype(jnp.float32), entering, precision=highest) * scaled[..., None]
    return (inner + carried).reshape(sequence_length, head_count, width)

def gated_norm(gated_rows, norm_scale, group_count):
    row_count = gated_rows.shape[0]
    widened = lax.optimization_barrier(gated_rows).astype(jnp.float32).reshape(row_count, group_count, -1)
    power = lax.optimization_barrier(jnp.mean(widened * widened, axis=-1, keepdims=True))
    return ((widened * lax.rsqrt(power + norm_eps)).reshape(row_count, -1) * norm_scale).astype(jnp.bfloat16)

def mamba(m_x, m_z, m_b, m_c, dt_raw, dt_bias, a_log, d_skip, norm_gain):
    sequence_length = m_x.shape[0]
    per_group = MH // MG
    x_all = m_x.reshape(sequence_length, MG, per_group, MP)
    step_all = jax.nn.softplus(dt_raw.astype(jnp.float32) + dt_bias).reshape(sequence_length, MG, per_group)
    rates = jnp.exp(a_log).reshape(MG, per_group)
    b_all = m_b.reshape(sequence_length, MG, MN)
    c_all = m_c.reshape(sequence_length, MG, MN)

    def by_group(packed):
        return ssd_sequence(packed[0], packed[1], packed[2], packed[3], packed[4])
    outputs = lax.map(by_group, (jnp.transpose(x_all, (1, 0, 2, 3)), jnp.transpose(step_all, (1, 0, 2)), rates, jnp.transpose(b_all, (1, 0, 2)), jnp.transpose(c_all, (1, 0, 2))))
    outputs = jnp.transpose(outputs, (1, 0, 2, 3)) + d_skip.reshape(MG, per_group)[None, :, :, None] * x_all.astype(jnp.float32)
    gated = (outputs.reshape(sequence_length, MH * MP) * jax.nn.silu(m_z.astype(jnp.float32))).astype(jnp.bfloat16)
    return gated_norm(gated, norm_gain, MG)

def reference(query, keys, values, m_x, m_z, m_b, m_c, dt_raw, dt_bias, a_log, d_skip, norm_gain):
    context = attention(folded_to_sequence(query), folded_to_sequence(keys), folded_to_sequence(values))
    mixed = mamba(folded_to_sequence(m_x), folded_to_sequence(m_z), folded_to_sequence(m_b), folded_to_sequence(m_c), folded_to_sequence(dt_raw), dt_bias, a_log, d_skip, norm_gain)
    return (context, mixed)
```

```python
import functools
import math

import jax
import jax.numpy as jnp
from jax import lax
from jax.experimental import pallas as pl
from jax.experimental.pallas import tpu as pltpu
from jax.sharding import PartitionSpec as P

HEAD_SIZE = 128
MP = 64
MN = 128
HALF = 64
TOK = 128
CTX = "ctx"
GRP_CTX = ("grp", "ctx")

norm_eps = 1e-05
F32 = jnp.float32
BF16 = jnp.bfloat16
NT = (((1,), (1,)), ((), ()))


def vmem_spec():
    return pl.BlockSpec(memory_space=pltpu.VMEM)


def smem_spec():
    return pl.BlockSpec(memory_space=pltpu.SMEM)


def any_spec():
    return pl.BlockSpec(memory_space=pl.ANY)


def cost(flops, moved):
    return pl.CostEstimate(flops=flops, bytes_accessed=moved, transcendentals=0)


def pack_kernel(k_ref, v_ref, b_ref, c_ref, dt_ref, out_ref):
    out_ref[0:128, :] = k_ref[...]
    out_ref[128:256, :] = v_ref[...]
    out_ref[256:384, :] = b_ref[...]
    out_ref[384:512, :] = c_ref[...]
    out_ref[512:, :] = dt_ref[...].astype(F32).T.astype(BF16)


def pack(keys, values, m_b, m_c, dt_raw):
    rows = 4 * TOK + dt_raw.shape[1]
    return pl.pallas_call(
        pack_kernel,
        out_shape=jax.ShapeDtypeStruct((rows, TOK), BF16),
        in_specs=[vmem_spec()] * 5,
        out_specs=vmem_spec(),
        cost_estimate=cost(10**6, 2 * rows * TOK * 2),
        name="pack",
    )(keys, values, m_b, m_c, dt_raw)


def turn_kernel(count, x_ref, z_ref, out_ref):
    width = x_ref.shape[1] // count
    per_tile = 128 // width
    for tile in range(x_ref.shape[1] // 128):
        columns = slice(tile * 128, tile * 128 + 128)
        for which, ref in enumerate((x_ref, z_ref)):
            turned = ref[:, columns].astype(F32).T.astype(BF16)
            for piece in range(per_tile):
                out_ref[tile * per_tile + piece, which * width : which * width + width, :] = turned[
                    piece * width : piece * width + width, :
                ]


def turn(m_x, m_z, count):
    width = m_x.shape[1] // count
    return pl.pallas_call(
        functools.partial(turn_kernel, count),
        out_shape=jax.ShapeDtypeStruct((count, 2 * width, TOK), BF16),
        in_specs=[vmem_spec()] * 2,
        out_specs=vmem_spec(),
        cost_estimate=cost(10**6, 4 * m_x.size * 2),
        name="turn",
    )(m_x, m_z)


def softplus(v):
    return jnp.maximum(v, 0.0) + jnp.log1p(jnp.exp(-jnp.abs(v)))


def ssd_kernel(count, g_ref, xz_ref, bias_ref, alog_ref, skip_ref, out_ref, bc, run_s, dt_s, end_s, tail_s, sem):
    copy = pltpu.make_async_copy(g_ref.at[:, 2 * TOK :, :], bc, sem)
    copy.start()
    copy.wait()
    width = xz_ref.shape[1] // 2
    me = lax.axis_index(CTX)
    head = (me * width) // MP
    bias, rate, skip = bias_ref[head], jnp.exp(jnp.full((1, 1), alog_ref[head], F32)), skip_ref[head]
    heads = bc.shape[1] - 2 * TOK
    lane = lax.broadcasted_iota(jnp.int32, (1, TOK), 1)
    low = lane < HALF
    mine = lax.broadcasted_iota(jnp.int32, (heads, TOK), 0) == head
    half_count = count // 2

    def dt_row(source):
        rows = bc[source, 2 * TOK :, :].astype(F32)
        return jnp.sum(jnp.where(mine, rows, 0.0), axis=0, keepdims=True)

    for m in range(half_count):
        first, second = dt_row(2 * m), dt_row(2 * m + 1)
        turned = pltpu.roll(second, HALF, 1)
        dt_s[m : m + 1, :] = jnp.where(low, first, turned)
        dt_s[count - 1 - m : count - m, :] = jnp.where(low, turned, first)
    dt = softplus(dt_s[...] + bias)
    dt_s[...] = dt
    run = -dt * rate
    lanes = lax.broadcasted_iota(jnp.int32, (count, TOK), 1)
    shift = 1
    while shift < TOK:
        run = run + jnp.where(lanes >= shift, pltpu.roll(run, shift, 1), 0.0)
        shift *= 2
    run_s[...] = run
    last = jnp.broadcast_to(run[:, TOK - 1 :], (count, TOK))
    end_s[...] = jnp.exp(last)
    tail_s[...] = jnp.exp(last - run) * dt
    row_id = lax.broadcasted_iota(jnp.int32, (TOK, TOK), 0)
    col_id = lax.broadcasted_iota(jnp.int32, (TOK, TOK), 1)
    seen = row_id <= col_id

    def chunk(k, state):
        early = k < half_count
        m = jnp.where(early, k, count - 1 - k)
        base = jnp.where(early, 0, HALF)
        one = jnp.where(early, 2 * m, 2 * m + 1)
        two = jnp.where(early, 2 * m + 1, 2 * m)

        def rows_of(offset):
            start = pl.multiple_of(base + offset, HALF)
            return jnp.concatenate([bc[one, pl.ds(start, HALF), :], bc[two, pl.ds(start, HALF), :]], axis=0)

        b_rows, c_rows = rows_of(0), rows_of(TOK)
        xz_even, xz_odd = xz_ref[2 * m].astype(F32), pltpu.roll(xz_ref[2 * m + 1].astype(F32), HALF, 1)
        xz = jnp.where(low == early, xz_even, xz_odd)
        x, z = xz[:width], xz[width:]
        run_row = jnp.broadcast_to(run_s[pl.ds(k, 1), :], (TOK, TOK))
        decay = jnp.exp(jnp.where(seen, run_row - run_row.T, -jnp.inf))
        cross = lax.dot_general(b_rows, c_rows, NT, preferred_element_type=F32)
        weights = (cross * decay).astype(BF16)
        x_dt = (x * dt_s[pl.ds(k, 1), :]).astype(BF16)
        inner = jnp.dot(x_dt, weights, preferred_element_type=F32)
        x_tail = (x * tail_s[pl.ds(k, 1), :]).astype(BF16)
        added = jnp.dot(x_tail, b_rows, preferred_element_type=F32)
        carried = lax.dot_general(state.astype(BF16), c_rows, NT, preferred_element_type=F32)
        y = inner + carried * jnp.exp(run_s[pl.ds(k, 1), :]) + skip * x
        gated = y * (z / (1.0 + jnp.exp(-z)))
        out_ref[k] = gated.astype(BF16)
        return state * end_s[pl.ds(k, 1), :] + added

    def chunks(step, state):
        for u in range(4):
            state = chunk(step * 4 + u, state)
        return state

    lax.fori_loop(0, count // 4, chunks, jnp.zeros((width, MN), F32))


def ssd(gathered, xz, dt_bias, a_log, d_skip):
    count, rows, _ = gathered.shape
    width = xz.shape[1] // 2
    return pl.pallas_call(
        functools.partial(ssd_kernel, count),
        out_shape=jax.ShapeDtypeStruct((count, width, TOK), BF16),
        in_specs=[any_spec(), vmem_spec(), smem_spec(), smem_spec(), smem_spec()],
        out_specs=vmem_spec(),
        scratch_shapes=[
            pltpu.VMEM((count, rows - 2 * TOK, TOK), BF16),
            pltpu.VMEM((count, TOK), F32),
            pltpu.VMEM((count, TOK), F32),
            pltpu.VMEM((count, TOK), F32),
            pltpu.VMEM((count, TOK), F32),
            pltpu.SemaphoreType.DMA,
        ],
        cost_estimate=cost(10**9, count * rows * TOK),
        name="ssd",
    )(gathered, xz, dt_bias, a_log, d_skip)


def attend_kernel(count, q0_ref, q1_ref, g_ref, out_ref, kv, q_s, m_s, l_s, acc_s, sem):
    copy = pltpu.make_async_copy(g_ref.at[:, : 2 * TOK, :], kv, sem)
    copy.start()
    heads = q0_ref.shape[1] // HEAD_SIZE
    for h in range(heads):
        columns = slice(h * HEAD_SIZE, (h + 1) * HEAD_SIZE)
        q_s[h * TOK : h * TOK + HALF, :] = q0_ref[:, columns]
        q_s[h * TOK + HALF : (h + 1) * TOK, :] = q1_ref[:, columns]
    m_s[...] = jnp.full(m_s.shape, -1e30, F32)
    l_s[...] = jnp.zeros(l_s.shape, F32)
    acc_s[...] = jnp.zeros(acc_s.shape, F32)
    me = lax.axis_index(CTX)
    scale = math.log2(math.e) / math.sqrt(HEAD_SIZE)
    copy.wait()
    blocks = 8
    rows = heads * TOK
    keys_here = blocks * HALF

    def step(index, masked):
        def piece(offset):
            parts = []
            for p in range(blocks):
                c = index * blocks + p
                early = c < count
                source = jnp.where(early, c, 2 * count - 1 - c)
                start = pl.multiple_of(jnp.where(early, 0, HALF) + offset, HALF)
                parts.append(kv[source, pl.ds(start, HALF), :])
            return jnp.concatenate(parts, axis=0)

        k_rows, v_rows = piece(0), piece(TOK)
        scores = lax.dot_general(q_s[...], k_rows, NT, preferred_element_type=F32)
        if masked:
            key_pos = index * keys_here + lax.broadcasted_iota(jnp.int32, (rows, keys_here), 1)
            row = lax.broadcasted_iota(jnp.int32, (rows, keys_here), 0)
            query_pos = me * TOK + jnp.bitwise_and(row, TOK - 1)
            scores = jnp.where(key_pos <= query_pos, scores, -1e30)
        old = m_s[...]
        new = jnp.maximum(old, jnp.max(scores, axis=1, keepdims=True))
        expons = jnp.exp2((scores - new) * scale)
        if masked:
            expons = jnp.where(key_pos <= query_pos, expons, 0.0)
        factor = jnp.exp2((old - new) * scale)
        m_s[...] = new
        l_s[...] = l_s[...] * factor + jnp.sum(expons, axis=1, keepdims=True)
        acc_s[...] = acc_s[...] * factor + jnp.dot(expons.astype(BF16), v_rows, preferred_element_type=F32)

    full = (me * TOK) // keys_here
    lax.fori_loop(0, full, lambda i, _: step(i, False), None)
    step(full, True)
    result = acc_s[...] / l_s[...]
    for h in range(heads):
        out_ref[:, h * HEAD_SIZE : (h + 1) * HEAD_SIZE] = result[h * TOK : (h + 1) * TOK, :].astype(BF16)


def attend(q0, q1, gathered):
    count, rows, _ = gathered.shape
    heads = q0.shape[1] // HEAD_SIZE
    return pl.pallas_call(
        functools.partial(attend_kernel, count),
        out_shape=jax.ShapeDtypeStruct((TOK, q0.shape[1]), BF16),
        in_specs=[vmem_spec(), vmem_spec(), any_spec()],
        out_specs=vmem_spec(),
        scratch_shapes=[
            pltpu.VMEM((count, 2 * TOK, TOK), BF16),
            pltpu.VMEM((heads * TOK, HEAD_SIZE), BF16),
            pltpu.VMEM((heads * TOK, 1), F32),
            pltpu.VMEM((heads * TOK, 1), F32),
            pltpu.VMEM((heads * TOK, HEAD_SIZE), F32),
            pltpu.SemaphoreType.DMA,
        ],
        cost_estimate=cost(4 * heads * TOK * count * TOK * HEAD_SIZE, count * rows * TOK),
        name="attend",
    )(q0, q1, gathered)


def norm_kernel(g_ref, gain_ref, out_ref):
    count, width, _ = g_ref.shape
    channels = count * width
    gated = g_ref[...].astype(F32).reshape(channels, TOK)
    power = jnp.sum(gated * gated, axis=0, keepdims=True) * (1.0 / channels)
    scaled = gated * lax.rsqrt(power + norm_eps)
    for tile in range(channels // 128):
        columns = slice(tile * 128, tile * 128 + 128)
        out_ref[:, columns] = (scaled[columns, :].T * gain_ref[:, columns]).astype(BF16)


def gated_norm(gated, gain):
    count, width, _ = gated.shape
    return pl.pallas_call(
        norm_kernel,
        out_shape=jax.ShapeDtypeStruct((TOK, count * width), BF16),
        in_specs=[vmem_spec()] * 2,
        out_specs=vmem_spec(),
        cost_estimate=cost(10**6, 4 * gated.size),
        name="norm",
    )(gated, gain.reshape(1, -1))


def body(query, keys, values, m_x, m_z, m_b, m_c, dt_raw, dt_bias, a_log, d_skip, norm_gain):
    count = lax.axis_size(CTX)
    me = lax.axis_index(CTX)
    gathered = lax.all_gather(pack(keys, values, m_b, m_c, dt_raw), CTX)
    xz = lax.all_to_all(turn(m_x, m_z, count), CTX, split_axis=0, concat_axis=0, tiled=True)

    parity = lax.rem(me, 2)
    block = [lambda d: d if d % 2 == 0 else 2 * count - 1 - d, lambda d: 2 * count - 1 - d if d % 2 == 0 else d]
    moved = []
    for slot in range(2):
        start = (parity if slot == 0 else 1 - parity) * HALF
        piece = lax.dynamic_slice_in_dim(query, start, HALF, 0)
        moved.append(lax.ppermute(piece, CTX, [(d, block[slot](d) // 2) for d in range(count)]))
    gated = ssd(gathered, xz, dt_bias, a_log, d_skip)
    returned = lax.all_to_all(gated, CTX, split_axis=0, concat_axis=0, tiled=True)
    context = attend(moved[0], moved[1], gathered)
    mixed = gated_norm(returned, norm_gain)
    return (context, mixed)


def solution(mesh):
    rows, heads = P(GRP_CTX, "hd"), P("hd")
    return jax.shard_map(
        body,
        mesh=mesh,
        in_specs=(rows,) * 8 + (heads,) * 4,
        out_specs=(rows, rows),
        check_vma=False,
    )
```

```python
import functools
import math

import jax
import jax.numpy as jnp
from jax import lax
from jax.experimental import pallas as pl
from jax.experimental.pallas import tpu as pltpu
from jax.sharding import PartitionSpec as P


HEAD_SIZE = 128
MP = 64
MN = 128
HALF = 64
TOK = 128
CTX = "ctx"
GRP_CTX = ("grp", "ctx")

norm_eps = 1e-05
F32 = jnp.float32
BF16 = jnp.bfloat16
NT = (((1,), (1,)), ((), ()))
TN = (((0,), (0,)), ((), ()))


SMALL = pltpu.CompilerParams(vmem_limit_bytes=16 * 2**20)


def vmem_spec():
    return pl.BlockSpec(memory_space=pltpu.VMEM)


def cost(flops, moved):
    return pl.CostEstimate(flops=flops, bytes_accessed=moved, transcendentals=0)


def is_first_core():
    return lax.rem(lax.axis_index(CTX), 2) == 0


def hbm_spec():
    return pl.BlockSpec(memory_space=pltpu.HBM)


def run_copies(pairs, sems):
    copies = [pltpu.make_async_copy(source, target, sems.at[i]) for i, (source, target) in enumerate(pairs)]
    for copy in copies:
        copy.start()
    return copies


def pack_kernel(k_ref, v_ref, out_ref, sems):
    for copy in run_copies([(k_ref, out_ref.at[:TOK]), (v_ref, out_ref.at[TOK:])], sems):
        copy.wait()


def pack(keys, values):
    return pl.pallas_call(
        pack_kernel,
        out_shape=jax.ShapeDtypeStruct((2 * TOK, HEAD_SIZE), BF16),
        in_specs=[hbm_spec()] * 2,
        out_specs=vmem_spec(),
        scratch_shapes=[pltpu.SemaphoreType.DMA((2,))],
        cost_estimate=cost(10**6, 8 * TOK * TOK),
        name="pack",
    )(keys, values)


def halves_kernel(
    x_ref, z_ref, b_ref, c_ref, dt_ref, bias_ref, alog_ref, skip_ref, mine_ref, theirs_ref, coef_ref, small, sems
):
    half = x_ref.shape[1] // 2
    tiles = half // 128
    heads = bias_ref.shape[0] // 2
    first = is_first_core()
    pairs = [(ref, small.at[i]) for i, ref in enumerate((bias_ref, alog_ref, skip_ref))]
    for out_ref, low in ((theirs_ref, jnp.logical_not(first)), (mine_ref, first)):
        base = jnp.where(low, 0, half)
        for which, ref in enumerate((x_ref, z_ref)):
            for t in range(tiles):
                row = (which * tiles + t) * TOK
                columns = pl.ds(pl.multiple_of(base + t * 128, 128), 128)
                pairs.append((ref.at[:, columns], out_ref.at[row : row + TOK]))
        row = 2 * tiles * TOK
        pairs.append((b_ref, out_ref.at[row : row + TOK]))
        pairs.append((c_ref, out_ref.at[row + TOK : row + 2 * TOK]))
        pairs.append((dt_ref, out_ref.at[row + 2 * TOK :]))
    copies = run_copies(pairs, sems)
    for copy in copies[:3]:
        copy.wait()
    head_row = lax.broadcasted_iota(jnp.int32, (heads, TOK), 0)
    at = jnp.where(first, 0, heads)
    bias, rate, skip = [jnp.zeros((heads, TOK), F32)] * 3
    for h in range(heads):
        bias = jnp.where(head_row == h, small[0, at + h], bias)
        rate = jnp.where(head_row == h, small[1, at + h], rate)
        skip = jnp.where(head_row == h, small[2, at + h], skip)
    rate = jnp.exp(rate)
    coef_ref[...] = jnp.concatenate([bias, bias, rate, rate, skip], axis=0)
    for copy in copies[3:]:
        copy.wait()


def halves(m_x, m_z, m_b, m_c, dt_turned, dt_bias, a_log, d_skip):
    rows = (m_x.shape[1] // 128 + 2) * TOK + dt_turned.shape[0]
    heads = dt_bias.shape[0] // 2
    tiles = m_x.shape[1] // 256
    shape = jax.ShapeDtypeStruct((rows, TOK), BF16)
    return pl.pallas_call(
        halves_kernel,
        out_shape=(shape, shape, jax.ShapeDtypeStruct((5 * heads, TOK), F32)),
        in_specs=[hbm_spec()] * 8,
        out_specs=(vmem_spec(),) * 3,
        scratch_shapes=[
            pltpu.SMEM((3, 2 * heads), F32),
            pltpu.SemaphoreType.DMA((3 + 2 * (2 * tiles + 3),)),
        ],
        cost_estimate=cost(10**6, 8 * rows * TOK),
        name="halves",
    )(m_x, m_z, m_b, m_c, dt_turned, dt_bias, a_log, d_skip)


def pair_of(mine_ref, got_ref, first, row):
    mine, got = mine_ref[row : row + TOK, :], got_ref[row : row + TOK, :]
    one, two = jnp.where(first, mine, got), jnp.where(first, got, mine)
    return (
        jnp.concatenate([one[:HALF], two[:HALF]], axis=0),
        jnp.concatenate([two[HALF:], one[HALF:]], axis=0),
    )


def softplus(v):
    return jnp.maximum(v, 0.0) + jnp.log1p(jnp.exp(-jnp.abs(v)))


def local_kernel(mine_ref, got_ref, coef_ref, states_ref, inner_ref, grown_ref):
    heads = coef_ref.shape[0] // 5
    tiles = heads * MP // 128
    first = is_first_core()
    row = 2 * tiles * TOK
    b_runs = pair_of(mine_ref, got_ref, first, row)
    c_runs = pair_of(mine_ref, got_ref, first, row + TOK)

    lane = lax.broadcasted_iota(jnp.int32, (heads, TOK), 1)
    low = lane < HALF
    mine_dt, got_dt = mine_ref[row + 2 * TOK :, :].astype(F32), got_ref[row + 2 * TOK :, :].astype(F32)
    mine_dt = jnp.where(first, mine_dt[:heads], mine_dt[heads:])
    got_dt = jnp.where(first, got_dt[:heads], got_dt[heads:])
    one, two = jnp.where(first, mine_dt, got_dt), jnp.where(first, got_dt, mine_dt)
    two = pltpu.roll(two, HALF, 1)
    raw = jnp.concatenate([jnp.where(low, one, two), jnp.where(low, two, one)], axis=0)
    bias, rate = coef_ref[: 2 * heads, :], coef_ref[2 * heads : 4 * heads, :]
    dt = softplus(raw + bias)
    run = -dt * rate
    lanes = lax.broadcasted_iota(jnp.int32, (2 * heads, TOK), 1)
    shift = 1
    while shift < TOK:
        run = run + jnp.where(lanes >= shift, pltpu.roll(run, shift, 1), 0.0)
        shift *= 2
    last = jnp.broadcast_to(run[:, TOK - 1 :], run.shape)
    tail = jnp.exp(last - run) * dt
    columns = jnp.concatenate([run, tail, jnp.zeros((TOK - 4 * heads, TOK), F32)], axis=0).T
    grown_ref[...] = jnp.exp(columns[:, : 2 * heads])
    high = last.astype(BF16)
    middle = (last - high.astype(F32)).astype(BF16)
    least = (last - high.astype(F32) - middle.astype(F32)).astype(BF16)
    parts = [part.astype(F32) for part in (high, middle, least)]

    row_id = lax.broadcasted_iota(jnp.int32, (TOK, TOK), 0)
    col_id = lax.broadcasted_iota(jnp.int32, (TOK, TOK), 1)
    seen = row_id >= col_id
    left = col_id < MP
    crosses = [lax.dot_general(c_runs[q], b_runs[q], NT, preferred_element_type=F32) for q in range(2)]
    for t in range(tiles):
        x_runs = pair_of(mine_ref, got_ref, first, t * TOK)
        for q in range(2):
            at = q * heads + 2 * t
            x = x_runs[q]
            wide = x.astype(F32)
            weights = []
            for e in range(2):
                spread = columns[:, at + e : at + e + 1] - run[at + e : at + e + 1, :]
                decay = jnp.exp(jnp.where(seen, spread, -jnp.inf))
                weights.append((crosses[q] * decay * dt[at + e : at + e + 1, :]).astype(BF16))
            both = jnp.dot(jnp.concatenate(weights, axis=0), x, preferred_element_type=F32)
            skip_row = 4 * heads + 2 * t
            skip = jnp.where(left, coef_ref[skip_row : skip_row + 1, :], coef_ref[skip_row + 1 : skip_row + 2, :])
            inner_ref[q, t] = jnp.where(left, both[:TOK], both[TOK:]) + skip * wide
            offset = 2 * heads + at
            tails = jnp.where(left, columns[:, offset : offset + 1], columns[:, offset + 1 : offset + 2])
            state = lax.dot_general((wide * tails).astype(BF16), b_runs[q], TN, preferred_element_type=F32)
            state = state.astype(BF16)
            for piece in range(4):
                states_ref[4 * t + piece, q * 32 : q * 32 + 32, :] = state[piece * 32 : piece * 32 + 32, :]
    part_row = lax.broadcasted_iota(jnp.int32, (8, TOK), 0)
    for h in range(heads):
        block = jnp.zeros((8, TOK), F32)
        for q in range(2):
            at = q * heads + h
            for i in range(3):
                block = jnp.where(part_row == 3 * q + i, parts[i][at : at + 1, :], block)
        for piece in range(2):
            states_ref[2 * h + piece, 64:72, :] = block.astype(BF16)


def local_states(mine, got, coef):
    heads = coef.shape[0] // 5
    width = heads * MP
    return pl.pallas_call(
        local_kernel,
        out_shape=(
            jax.ShapeDtypeStruct((width // 32, 72, MN), BF16),
            jax.ShapeDtypeStruct((2, width // 128, TOK, 128), F32),
            jax.ShapeDtypeStruct((TOK, 2 * heads), F32),
        ),
        in_specs=[vmem_spec()] * 3,
        out_specs=(vmem_spec(), vmem_spec(), vmem_spec()),
        compiler_params=SMALL,
        cost_estimate=cost(10**9, 10**6),
        name="local",
    )(mine, got, coef)


def chain_kernel(states_ref, out_ref):
    count = states_ref.shape[0]
    state = jnp.zeros((32, MN), F32)
    for q in range(2):
        for k in range(count) if q == 0 else reversed(range(count)):
            out_ref[k, q * 32 : q * 32 + 32, :] = state.astype(BF16)
            parts = states_ref[k, 64:72, :].astype(F32)
            decay = jnp.exp(parts[3 * q : 3 * q + 1] + parts[3 * q + 1 : 3 * q + 2] + parts[3 * q + 2 : 3 * q + 3])
            state = state * decay + states_ref[k, q * 32 : q * 32 + 32, :].astype(F32)


def chain(states):
    count = states.shape[0]
    return pl.pallas_call(
        chain_kernel,
        out_shape=jax.ShapeDtypeStruct((count, 64, MN), BF16),
        in_specs=[vmem_spec()],
        out_specs=vmem_spec(),
        compiler_params=SMALL,
        cost_estimate=cost(10**6, 10**6),
        name="chain",
    )(states)


def gate_kernel(entering_ref, inner_ref, grown_ref, mine_ref, got_ref, even_ref, odd_ref):
    tiles = inner_ref.shape[1]
    heads = 2 * tiles
    first = is_first_core()
    c_runs = pair_of(mine_ref, got_ref, first, (2 * tiles + 1) * TOK)
    left = lax.broadcasted_iota(jnp.int32, (TOK, 128), 1) < MP
    for t in range(tiles):
        z_runs = pair_of(mine_ref, got_ref, first, (tiles + t) * TOK)
        results = []
        for q in range(2):
            at = q * heads + 2 * t
            state = entering_ref[4 * t : 4 * t + 4, q * 32 : q * 32 + 32, :].reshape(128, MN)
            carried = lax.dot_general(c_runs[q], state, NT, preferred_element_type=F32)
            grown = jnp.where(left, grown_ref[:, at : at + 1], grown_ref[:, at + 1 : at + 2])
            y = inner_ref[q, t] + carried * grown
            z = z_runs[q].astype(F32)
            results.append((y * (z / (1.0 + jnp.exp(-z)))).astype(BF16))
        even_ref[:, t * 128 : t * 128 + 128] = jnp.where(first, results[0], results[1])
        odd_ref[:, t * 128 : t * 128 + 128] = jnp.where(first, results[1], results[0])


def gate(entering, inner, grown, mine, got):
    shape = jax.ShapeDtypeStruct((TOK, inner.shape[1] * 128), BF16)
    return pl.pallas_call(
        gate_kernel,
        out_shape=(shape, shape),
        in_specs=[vmem_spec()] * 5,
        out_specs=(vmem_spec(), vmem_spec()),
        compiler_params=SMALL,
        cost_estimate=cost(10**8, 10**6),
        name="gate",
    )(entering, inner, grown, mine, got)


def norm_kernel(half_count, even_ref, odd_ref, gain_ref, out_ref):
    early = lax.axis_index(CTX) < half_count
    width = even_ref.shape[1]
    even, odd = even_ref[...], odd_ref[...]
    one = jnp.where(early, even, odd).astype(F32)
    two = jnp.where(early, odd, even).astype(F32)
    power = jnp.sum(one * one + two * two, axis=1, keepdims=True) * (0.5 / width)
    scale = lax.rsqrt(power + norm_eps)
    out_ref[:, :width] = ((one * scale) * gain_ref[:, :width]).astype(BF16)
    out_ref[:, width:] = ((two * scale) * gain_ref[:, width:]).astype(BF16)


def gated_norm(even, odd, gain, half_count):
    return pl.pallas_call(
        functools.partial(norm_kernel, half_count),
        out_shape=jax.ShapeDtypeStruct((TOK, 2 * even.shape[1]), BF16),
        in_specs=[vmem_spec()] * 3,
        out_specs=vmem_spec(),
        compiler_params=SMALL,
        cost_estimate=cost(10**6, 10**6),
        name="norm",
    )(even, odd, gain.reshape(1, -1))


def attend_kernel(count, q0_ref, q1_ref, g_ref, out_ref, kv, q_s, m_s, l_s, acc_s, sems):
    blocks = 8
    parts = count // blocks
    copies = run_copies(
        [(g_ref.at[part * blocks : (part + 1) * blocks], kv.at[part * blocks : (part + 1) * blocks]) for part in range(parts)],
        sems,
    )
    heads = q0_ref.shape[1] // HEAD_SIZE
    for h in range(heads):
        columns = slice(h * HEAD_SIZE, (h + 1) * HEAD_SIZE)
        q_s[h * TOK : h * TOK + HALF, :] = q0_ref[:, columns]
        q_s[h * TOK + HALF : (h + 1) * TOK, :] = q1_ref[:, columns]
    m_s[...] = jnp.full(m_s.shape, -1e30, F32)
    l_s[...] = jnp.zeros(l_s.shape, F32)
    acc_s[...] = jnp.zeros(acc_s.shape, F32)
    me = lax.axis_index(CTX)
    scale = math.log2(math.e) / math.sqrt(HEAD_SIZE)
    rows = heads * TOK
    keys_here = blocks * HALF

    def step(index, masked):
        def piece(offset):
            parts = []
            for p in range(blocks):
                c = index * blocks + p
                early = c < count
                source = jnp.where(early, c, 2 * count - 1 - c)
                start = pl.multiple_of(jnp.where(early, 0, HALF) + offset, HALF)
                parts.append(kv[source, pl.ds(start, HALF), :])
            return jnp.concatenate(parts, axis=0)

        k_rows, v_rows = piece(0), piece(TOK)
        scores = lax.dot_general(k_rows, q_s[...], NT, preferred_element_type=F32)
        if masked:
            key_pos = index * keys_here + lax.broadcasted_iota(jnp.int32, (keys_here, rows), 0)
            column = lax.broadcasted_iota(jnp.int32, (keys_here, rows), 1)
            query_pos = me * TOK + jnp.bitwise_and(column, TOK - 1)
            scores = jnp.where(key_pos <= query_pos, scores, -1e30)
        old = m_s[...]
        new = jnp.maximum(old, jnp.max(scores, axis=0, keepdims=True))
        expons = jnp.exp2((scores - new) * scale)
        if masked:
            expons = jnp.where(key_pos <= query_pos, expons, 0.0)
        factor = jnp.exp2((old - new) * scale)
        m_s[...] = new
        l_s[...] = l_s[...] * factor + jnp.sum(expons, axis=0, keepdims=True)
        acc_s[...] = acc_s[...] * factor + lax.dot_general(
            v_rows, expons.astype(BF16), TN, preferred_element_type=F32
        )

    full = (me * TOK) // keys_here

    def arrived(index):
        for part in range(parts):

            @pl.when(index == part)
            def _():
                copies[part].wait()

    def whole_step(index, _):
        arrived(index)
        step(index, False)

    lax.fori_loop(0, full, whole_step, None)
    arrived(full)
    step(full, True)
    for part in range(parts):

        @pl.when(full < part)
        def _():
            copies[part].wait()

    result = acc_s[...] / l_s[...]
    for h in range(heads):
        columns = slice(h * TOK, (h + 1) * TOK)
        out_ref[:, h * HEAD_SIZE : (h + 1) * HEAD_SIZE] = result[:, columns].T.astype(BF16)


def attend(q0, q1, gathered):
    count, rows, _ = gathered.shape
    heads = q0.shape[1] // HEAD_SIZE
    return pl.pallas_call(
        functools.partial(attend_kernel, count),
        out_shape=jax.ShapeDtypeStruct((TOK, q0.shape[1]), BF16),
        in_specs=[vmem_spec(), vmem_spec(), hbm_spec()],
        out_specs=vmem_spec(),
        scratch_shapes=[
            pltpu.VMEM((count, rows, TOK), BF16),
            pltpu.VMEM((heads * TOK, HEAD_SIZE), BF16),
            pltpu.VMEM((1, heads * TOK), F32),
            pltpu.VMEM((1, heads * TOK), F32),
            pltpu.VMEM((HEAD_SIZE, heads * TOK), F32),
            pltpu.SemaphoreType.DMA((count // 8,)),
        ],
        cost_estimate=cost(4 * heads * TOK * count * TOK * HEAD_SIZE, count * rows * TOK),
        name="attend",
    )(q0, q1, gathered)


def permute(value, count, target):
    return lax.ppermute(value, CTX, [(d, target(d)) for d in range(count)])


def layer(query, keys, values, m_x, m_z, m_b, m_c, dt_raw, dt_bias, a_log, d_skip, norm_gain):
    count = lax.axis_size(CTX)
    chips = count // 2
    gathered = lax.all_gather(pack(keys, values), CTX)

    mine, theirs, coef = halves(m_x, m_z, m_b, m_c, dt_raw.T, dt_bias, a_log, d_skip)
    got = permute(theirs, count, lambda d: d ^ 1)
    states, inner, grown = local_states(mine, got, coef)
    same_core = [list(range(core, count, 2)) for core in range(2)]
    exchange = functools.partial(
        lax.all_to_all, axis_name=CTX, split_axis=0, concat_axis=0, tiled=True, axis_index_groups=same_core
    )
    parity = lax.rem(lax.axis_index(CTX), 2)
    block = [lambda d: d if d % 2 == 0 else 2 * count - 1 - d, lambda d: 2 * count - 1 - d if d % 2 == 0 else d]
    queries = []
    for slot in range(2):
        start = (parity if slot == 0 else 1 - parity) * HALF
        piece = lax.dynamic_slice_in_dim(query, start, HALF, 0)
        queries.append(permute(piece, count, lambda d: block[slot](d) // 2))
    exchanged = exchange(states)
    entering = exchange(chain(exchanged))

    even, odd = gate(entering, inner, grown, mine, got)
    even = permute(even, count, lambda d: d // 2 if d % 2 == 0 else count - 1 - d // 2)
    odd = permute(odd, count, lambda d: count - 1 - d // 2 if d % 2 == 0 else d // 2)
    context = attend(queries[0], queries[1], gathered)
    even, odd, context = lax.optimization_barrier((even, odd, context))
    mixed = gated_norm(even, odd, norm_gain, chips)
    return (context, mixed)


def solution(mesh):
    rows, heads = P(GRP_CTX, "hd"), P("hd")
    return jax.shard_map(
        layer,
        mesh=mesh,
        in_specs=(rows,) * 8 + (heads,) * 4,
        out_specs=(rows, rows),
        check_vma=False,
    )
```

```python
import functools
import math

import jax
import jax.numpy as jnp
from jax import lax
from jax.experimental import pallas as pl
from jax.experimental.pallas import tpu as pltpu
from jax.sharding import PartitionSpec as P


HEAD_SIZE = 128
MP = 64
MN = 128
HALF = 64
TOK = 128
CTX = "ctx"
GRP_CTX = ("grp", "ctx")

norm_eps = 1e-05
F32 = jnp.float32
BF16 = jnp.bfloat16
NT = (((1,), (1,)), ((), ()))
TN = (((0,), (0,)), ((), ()))


SMALL = pltpu.CompilerParams(vmem_limit_bytes=16 * 2**20)


def vmem_spec():
    return pl.BlockSpec(memory_space=pltpu.VMEM)


def cost(flops, moved):
    return pl.CostEstimate(flops=flops, bytes_accessed=moved, transcendentals=0)


def is_first_core():
    return lax.rem(lax.axis_index(CTX), 2) == 0


def hbm_spec():
    return pl.BlockSpec(memory_space=pltpu.HBM)


def run_copies(pairs, sems):
    copies = [pltpu.make_async_copy(source, target, sems.at[i]) for i, (source, target) in enumerate(pairs)]
    for copy in copies:
        copy.start()
    return copies


def halves_kernel(*refs):
    x_ref, z_ref, b_ref, c_ref, dt_ref, k_ref, v_ref, q_ref, bias_ref, alog_ref, skip_ref = refs[:11]
    mine_ref, theirs_ref, kv_ref, even_ref, odd_ref, small, sems = refs[11:]
    half = x_ref.shape[1] // 2
    tiles = half // 128
    heads = bias_ref.shape[0] // 2
    first = is_first_core()
    pairs = [(ref, small.at[i]) for i, ref in enumerate((bias_ref, alog_ref, skip_ref))]
    pairs += [(k_ref, kv_ref.at[:TOK]), (v_ref, kv_ref.at[TOK:])]
    for out_ref, low in ((theirs_ref, jnp.logical_not(first)), (mine_ref, first)):
        base = jnp.where(low, 0, half)
        for which, ref in enumerate((x_ref, z_ref)):
            for t in range(tiles):
                row = (which * tiles + t) * TOK
                columns = pl.ds(pl.multiple_of(base + t * 128, 128), 128)
                pairs.append((ref.at[:, columns], out_ref.at[row : row + TOK]))
        row = 2 * tiles * TOK
        pairs.append((b_ref, out_ref.at[row : row + TOK]))
        pairs.append((c_ref, out_ref.at[row + TOK : row + 2 * TOK]))
        pairs.append((dt_ref, out_ref.at[row + 2 * TOK : row + 2 * TOK + 2 * heads]))
    for out_ref, low in ((even_ref, first), (odd_ref, jnp.logical_not(first))):
        start = pl.multiple_of(jnp.where(low, 0, HALF), HALF)
        pairs.append((q_ref.at[pl.ds(start, HALF), :], out_ref))
    copies = run_copies(pairs, sems)
    for copy in copies[:3]:
        copy.wait()
    head_row = lax.broadcasted_iota(jnp.int32, (heads, TOK), 0)
    at = jnp.where(first, 0, heads)
    bias, rate, skip = [jnp.zeros((heads, TOK), F32)] * 3
    for h in range(heads):
        bias = jnp.where(head_row == h, small[0, at + h], bias)
        rate = jnp.where(head_row == h, small[1, at + h], rate)
        skip = jnp.where(head_row == h, small[2, at + h], skip)
    rate = jnp.exp(rate)
    rest = jnp.concatenate([bias, bias, rate, rate, skip, skip], axis=0)
    start = row + 2 * TOK + 2 * heads
    for part in range(3):
        rounded = rest.astype(BF16)
        mine_ref[start + part * 6 * heads : start + (part + 1) * 6 * heads, :] = rounded
        rest = rest - rounded.astype(F32)
    for copy in copies[3:]:
        copy.wait()


def halves(m_x, m_z, m_b, m_c, dt_turned, keys, values, query, dt_bias, a_log, d_skip):
    heads = dt_bias.shape[0] // 2
    rows = (m_x.shape[1] // 128 + 2) * TOK + 2 * heads
    tiles = m_x.shape[1] // 256
    half_query = jax.ShapeDtypeStruct((HALF, query.shape[1]), BF16)
    return pl.pallas_call(
        halves_kernel,
        out_shape=(
            jax.ShapeDtypeStruct((rows + 18 * heads, TOK), BF16),
            jax.ShapeDtypeStruct((rows, TOK), BF16),
            jax.ShapeDtypeStruct((2 * TOK, HEAD_SIZE), BF16),
            half_query,
            half_query,
        ),
        in_specs=[hbm_spec()] * 11,
        out_specs=(vmem_spec(),) * 5,
        scratch_shapes=[
            pltpu.SMEM((3, 2 * heads), F32),
            pltpu.SemaphoreType.DMA((5 + 2 * (2 * tiles + 3) + 2,)),
        ],
        cost_estimate=cost(10**6, 8 * rows * TOK),
        name="halves",
    )(m_x, m_z, m_b, m_c, dt_turned, keys, values, query, dt_bias, a_log, d_skip)


def pair_of(mine_ref, got_ref, first, row):
    mine, got = mine_ref[row : row + TOK, :], got_ref[row : row + TOK, :]
    one, two = jnp.where(first, mine, got), jnp.where(first, got, mine)
    return (
        jnp.concatenate([one[:HALF], two[:HALF]], axis=0),
        jnp.concatenate([two[HALF:], one[HALF:]], axis=0),
    )


def softplus(v):
    return jnp.maximum(v, 0.0) + jnp.log1p(jnp.exp(-jnp.abs(v)))


def local_kernel(mine_ref, got_ref, states_ref, inner_ref, grown_ref):
    heads = (mine_ref.shape[0] - got_ref.shape[0]) // 18
    tiles = heads * MP // 128
    first = is_first_core()
    row = 2 * tiles * TOK
    b_runs = pair_of(mine_ref, got_ref, first, row)
    c_runs = pair_of(mine_ref, got_ref, first, row + TOK)

    lane = lax.broadcasted_iota(jnp.int32, (heads, TOK), 1)
    low = lane < HALF
    dt_rows = slice(row + 2 * TOK, row + 2 * TOK + 2 * heads)
    mine_dt, got_dt = mine_ref[dt_rows, :].astype(F32), got_ref[dt_rows, :].astype(F32)
    coef = sum(
        mine_ref[dt_rows.stop + part * 6 * heads : dt_rows.stop + (part + 1) * 6 * heads, :].astype(F32) for part in range(3)
    )
    mine_dt = jnp.where(first, mine_dt[:heads], mine_dt[heads:])
    got_dt = jnp.where(first, got_dt[:heads], got_dt[heads:])
    one, two = jnp.where(first, mine_dt, got_dt), jnp.where(first, got_dt, mine_dt)
    two = pltpu.roll(two, HALF, 1)
    raw = jnp.concatenate([jnp.where(low, one, two), jnp.where(low, two, one)], axis=0)
    bias, rate = coef[: 2 * heads, :], coef[2 * heads : 4 * heads, :]
    dt = softplus(raw + bias)
    run = -dt * rate
    lanes = lax.broadcasted_iota(jnp.int32, (2 * heads, TOK), 1)
    shift = 1
    while shift < TOK:
        run = run + jnp.where(lanes >= shift, pltpu.roll(run, shift, 1), 0.0)
        shift *= 2
    last = jnp.broadcast_to(run[:, TOK - 1 :], run.shape)
    tail = jnp.exp(last - run) * dt
    columns = jnp.concatenate([run, tail, jnp.zeros((TOK - 4 * heads, TOK), F32)], axis=0).T
    grown_ref[...] = jnp.exp(columns[:, : 2 * heads])
    high = last.astype(BF16)
    middle = (last - high.astype(F32)).astype(BF16)
    least = (last - high.astype(F32) - middle.astype(F32)).astype(BF16)
    parts = [part.astype(F32) for part in (high, middle, least)]

    row_id = lax.broadcasted_iota(jnp.int32, (TOK, TOK), 0)
    col_id = lax.broadcasted_iota(jnp.int32, (TOK, TOK), 1)
    seen = row_id >= col_id
    left = col_id < MP
    crosses = [lax.dot_general(c_runs[q], b_runs[q], NT, preferred_element_type=F32) for q in range(2)]
    for t in range(tiles):
        x_runs = pair_of(mine_ref, got_ref, first, t * TOK)
        for q in range(2):
            at = q * heads + 2 * t
            x = x_runs[q]
            wide = x.astype(F32)
            weights = []
            for e in range(2):
                spread = columns[:, at + e : at + e + 1] - run[at + e : at + e + 1, :]
                decay = jnp.exp(jnp.where(seen, spread, -jnp.inf))
                weights.append((crosses[q] * decay * dt[at + e : at + e + 1, :]).astype(BF16))
            both = jnp.dot(jnp.concatenate(weights, axis=0), x, preferred_element_type=F32)
            skip_row = 4 * heads + 2 * t
            skip = jnp.where(left, coef[skip_row : skip_row + 1, :], coef[skip_row + 1 : skip_row + 2, :])
            inner_ref[q, t] = jnp.where(left, both[:TOK], both[TOK:]) + skip * wide
            offset = 2 * heads + at
            tails = jnp.where(left, columns[:, offset : offset + 1], columns[:, offset + 1 : offset + 2])
            state = lax.dot_general((wide * tails).astype(BF16), b_runs[q], TN, preferred_element_type=F32)
            state = state.astype(BF16)
            for piece in range(4):
                states_ref[4 * t + piece, q * 32 : q * 32 + 32, :] = state[piece * 32 : piece * 32 + 32, :]
    part_row = lax.broadcasted_iota(jnp.int32, (8, TOK), 0)
    for h in range(heads):
        block = jnp.zeros((8, TOK), F32)
        for q in range(2):
            at = q * heads + h
            for i in range(3):
                block = jnp.where(part_row == 3 * q + i, parts[i][at : at + 1, :], block)
        for piece in range(2):
            states_ref[2 * h + piece, 64:72, :] = block.astype(BF16)


def local_states(mine, got):
    heads = (mine.shape[0] - got.shape[0]) // 18
    width = heads * MP
    return pl.pallas_call(
        local_kernel,
        out_shape=(
            jax.ShapeDtypeStruct((width // 32, 72, MN), BF16),
            jax.ShapeDtypeStruct((2, width // 128, TOK, 128), F32),
            jax.ShapeDtypeStruct((TOK, 2 * heads), F32),
        ),
        in_specs=[vmem_spec()] * 2,
        out_specs=(vmem_spec(), vmem_spec(), vmem_spec()),
        compiler_params=SMALL,
        cost_estimate=cost(10**9, 10**6),
        name="local",
    )(mine, got)


def chain_kernel(states_ref, out_ref):
    count = states_ref.shape[0]
    state = jnp.zeros((32, MN), F32)
    for q in range(2):
        for k in range(count) if q == 0 else reversed(range(count)):
            out_ref[k, q * 32 : q * 32 + 32, :] = state.astype(BF16)
            parts = states_ref[k, 64:72, :].astype(F32)
            decay = jnp.exp(parts[3 * q : 3 * q + 1] + parts[3 * q + 1 : 3 * q + 2] + parts[3 * q + 2 : 3 * q + 3])
            state = state * decay + states_ref[k, q * 32 : q * 32 + 32, :].astype(F32)


def chain(states):
    count = states.shape[0]
    return pl.pallas_call(
        chain_kernel,
        out_shape=jax.ShapeDtypeStruct((count, 64, MN), BF16),
        in_specs=[vmem_spec()],
        out_specs=vmem_spec(),
        compiler_params=SMALL,
        cost_estimate=cost(10**6, 10**6),
        name="chain",
    )(states)


def gate_kernel(entering_ref, inner_ref, grown_ref, mine_ref, got_ref, even_ref, odd_ref):
    tiles = inner_ref.shape[1]
    heads = 2 * tiles
    first = is_first_core()
    c_runs = pair_of(mine_ref, got_ref, first, (2 * tiles + 1) * TOK)
    left = lax.broadcasted_iota(jnp.int32, (TOK, 128), 1) < MP
    for t in range(tiles):
        z_runs = pair_of(mine_ref, got_ref, first, (tiles + t) * TOK)
        results = []
        for q in range(2):
            at = q * heads + 2 * t
            state = entering_ref[4 * t : 4 * t + 4, q * 32 : q * 32 + 32, :].reshape(128, MN)
            carried = lax.dot_general(c_runs[q], state, NT, preferred_element_type=F32)
            grown = jnp.where(left, grown_ref[:, at : at + 1], grown_ref[:, at + 1 : at + 2])
            y = inner_ref[q, t] + carried * grown
            z = z_runs[q].astype(F32)
            results.append((y * (z / (1.0 + jnp.exp(-z)))).astype(BF16))
        even_ref[:, t * 128 : t * 128 + 128] = jnp.where(first, results[0], results[1])
        odd_ref[:, t * 128 : t * 128 + 128] = jnp.where(first, results[1], results[0])


def gate(entering, inner, grown, mine, got):
    shape = jax.ShapeDtypeStruct((TOK, inner.shape[1] * 128), BF16)
    return pl.pallas_call(
        gate_kernel,
        out_shape=(shape, shape),
        in_specs=[vmem_spec()] * 5,
        out_specs=(vmem_spec(), vmem_spec()),
        compiler_params=SMALL,
        cost_estimate=cost(10**8, 10**6),
        name="gate",
    )(entering, inner, grown, mine, got)


def norm_kernel(half_count, even_ref, odd_ref, even_far_ref, odd_far_ref, gain_ref, out_ref):
    early = lax.axis_index(CTX) < half_count
    width = even_ref.shape[1]
    even, odd = even_ref[...] + even_far_ref[...], odd_ref[...] + odd_far_ref[...]
    one = jnp.where(early, even, odd).astype(F32)
    two = jnp.where(early, odd, even).astype(F32)
    power = jnp.sum(one * one + two * two, axis=1, keepdims=True) * (0.5 / width)
    scale = lax.rsqrt(power + norm_eps)
    out_ref[:, :width] = ((one * scale) * gain_ref[:, :width]).astype(BF16)
    out_ref[:, width:] = ((two * scale) * gain_ref[:, width:]).astype(BF16)


def gated_norm(even, odd, even_far, odd_far, gain, half_count):
    return pl.pallas_call(
        functools.partial(norm_kernel, half_count),
        out_shape=jax.ShapeDtypeStruct((TOK, 2 * even.shape[1]), BF16),
        in_specs=[vmem_spec()] * 5,
        out_specs=vmem_spec(),
        compiler_params=SMALL,
        cost_estimate=cost(10**6, 10**6),
        name="norm",
    )(even, odd, even_far, odd_far, gain.reshape(1, -1))


def attend_kernel(count, q0_ref, q1_ref, g_ref, out_ref, kv, q_s, m_s, l_s, acc_s, sems):
    blocks = 8
    parts = count // blocks
    me = lax.axis_index(CTX)
    keys_here = blocks * HALF
    full = (me * TOK) // keys_here
    copies = []
    for part in range(parts):
        of_part = slice(part * blocks, (part + 1) * blocks)
        copies.append(pltpu.make_async_copy(g_ref.at[of_part], kv.at[of_part], sems.at[part]))

        @pl.when(part <= full)
        def _():
            copies[part].start()

    heads = q0_ref.shape[1] // HEAD_SIZE
    for h in range(heads):
        columns = slice(h * HEAD_SIZE, (h + 1) * HEAD_SIZE)
        q_s[h * TOK : h * TOK + HALF, :] = q0_ref[:, columns]
        q_s[h * TOK + HALF : (h + 1) * TOK, :] = q1_ref[:, columns]
    m_s[...] = jnp.full(m_s.shape, -1e30, F32)
    l_s[...] = jnp.zeros(l_s.shape, F32)
    acc_s[...] = jnp.zeros(acc_s.shape, F32)
    scale = math.log2(math.e) / math.sqrt(HEAD_SIZE)
    rows = heads * TOK

    def step(first_block, block_count, diagonal):
        def piece(offset):
            parts = []
            for p in range(block_count):
                c = first_block + p
                early = c < count
                source = jnp.where(early, c, 2 * count - 1 - c)
                start = pl.multiple_of(jnp.where(early, 0, HALF) + offset, HALF)
                parts.append(kv[source, pl.ds(start, HALF), :])
            return jnp.concatenate(parts, axis=0)

        k_rows, v_rows = piece(0), piece(TOK)
        scores = lax.dot_general(k_rows, q_s[...], NT, preferred_element_type=F32)
        if diagonal:
            key = lax.broadcasted_iota(jnp.int32, (TOK, rows), 0)
            column = lax.broadcasted_iota(jnp.int32, (TOK, rows), 1)
            seen = key <= jnp.bitwise_and(column, TOK - 1)
            scores = jnp.where(seen, scores, -1e30)
        old = m_s[...]
        new = jnp.maximum(old, jnp.max(scores, axis=0, keepdims=True))
        expons = jnp.exp2((scores - new) * scale)
        if diagonal:
            expons = jnp.where(seen, expons, 0.0)
        factor = jnp.exp2((old - new) * scale)
        m_s[...] = new
        l_s[...] = l_s[...] * factor + jnp.sum(expons, axis=0, keepdims=True)
        acc_s[...] = acc_s[...] * factor + lax.dot_general(
            v_rows, expons.astype(BF16), TN, preferred_element_type=F32
        )

    def arrived(index):
        for part in range(parts):

            @pl.when(index == part)
            def _():
                copies[part].wait()

    def whole_step(index, _):
        arrived(index)
        step(index * blocks, blocks, False)

    lax.fori_loop(0, full, whole_step, None)
    arrived(full)
    left = lax.rem(me * TOK, keys_here) // TOK
    for whole in range(1, keys_here // TOK):

        @pl.when(left == whole)
        def _():
            step(full * blocks, 2 * whole, False)

    step(2 * me, 2, True)
    result = acc_s[...] / l_s[...]
    for h in range(heads):
        columns = slice(h * TOK, (h + 1) * TOK)
        out_ref[:, h * HEAD_SIZE : (h + 1) * HEAD_SIZE] = result[:, columns].T.astype(BF16)


def attend(q0, q1, gathered):
    count, rows, _ = gathered.shape
    heads = q0.shape[1] // HEAD_SIZE
    return pl.pallas_call(
        functools.partial(attend_kernel, count),
        out_shape=jax.ShapeDtypeStruct((TOK, q0.shape[1]), BF16),
        in_specs=[vmem_spec(), vmem_spec(), hbm_spec()],
        out_specs=vmem_spec(),
        scratch_shapes=[
            pltpu.VMEM((count, rows, TOK), BF16),
            pltpu.VMEM((heads * TOK, HEAD_SIZE), BF16),
            pltpu.VMEM((1, heads * TOK), F32),
            pltpu.VMEM((1, heads * TOK), F32),
            pltpu.VMEM((HEAD_SIZE, heads * TOK), F32),
            pltpu.SemaphoreType.DMA((count // 8,)),
        ],
        cost_estimate=cost(4 * heads * TOK * count * TOK * HEAD_SIZE, count * rows * TOK),
        name="attend",
    )(q0, q1, gathered)


def permute(value, target, sources):
    return lax.ppermute(value, CTX, [(d, target(d)) for d in sources])


RELAY_HOPS = 7
RESULT_RELAYS = 1


def relay(value, count, chips):
    sources = range(count - 2 * chips, count)
    return permute(value, lambda d: (d + 2 * RELAY_HOPS) % count, sources)


def forward(value, count, chips, target):
    sources = range(count - 2 * chips, count)
    return lax.ppermute(value, CTX, [((d + 2 * RELAY_HOPS) % count, target(d)) for d in sources])


def layer(query, keys, values, m_x, m_z, m_b, m_c, dt_raw, dt_bias, a_log, d_skip, norm_gain):
    count = lax.axis_size(CTX)
    chips = count // 2
    mine, theirs, pairs, *pieces = halves(
        m_x, m_z, m_b, m_c, dt_raw.T, keys, values, query, dt_bias, a_log, d_skip
    )
    gathered = lax.all_gather(pairs, CTX)
    got = permute(theirs, lambda d: d ^ 1, range(count))
    states, inner, grown = local_states(mine, got)
    same_core = [list(range(core, count, 2)) for core in range(2)]
    exchange = functools.partial(
        lax.all_to_all, axis_name=CTX, split_axis=0, concat_axis=0, tiled=True, axis_index_groups=same_core
    )
    block = [lambda d: d if d % 2 == 0 else 2 * count - 1 - d, lambda d: 2 * count - 1 - d if d % 2 == 0 else d]
    queries = []
    for slot in range(2):
        queries.append(permute(pieces[slot], lambda d: block[slot](d) // 2, range(count)))
    exchanged = exchange(states)
    entering = exchange(chain(exchanged))

    even, odd = gate(entering, inner, grown, mine, got)
    goals = [
        lambda d: d // 2 if d % 2 == 0 else count - 1 - d // 2,
        lambda d: count - 1 - d // 2 if d % 2 == 0 else d // 2,
    ]
    results = (even, odd)
    direct = [permute(results[slot], goals[slot], range(count - 2 * RESULT_RELAYS)) for slot in range(2)]
    relayed = [relay(results[slot], count, RESULT_RELAYS) for slot in range(2)]
    ahead = [forward(relayed[slot], count, RESULT_RELAYS, goals[slot]) for slot in range(2)]
    context = attend(queries[0], queries[1], gathered)
    direct, ahead, context = lax.optimization_barrier((direct, ahead, context))
    mixed = gated_norm(*direct, *ahead, norm_gain, chips)
    return (context, mixed)


def solution(mesh):
    rows, heads = P(GRP_CTX, "hd"), P("hd")
    return jax.shard_map(
        layer,
        mesh=mesh,
        in_specs=(rows,) * 8 + (heads,) * 4,
        out_specs=(rows, rows),
        check_vma=False,
    )
```

```python
import functools
import math

import jax
import jax.numpy as jnp
from jax import lax
from jax.experimental import pallas as pl
from jax.experimental.pallas import tpu as pltpu
from jax.sharding import PartitionSpec as P


HEAD_SIZE = 128
MP = 64
MN = 128
HALF = 64
TOK = 128
CTX = "ctx"
GRP_CTX = ("grp", "ctx")

norm_eps = 1e-05
F32 = jnp.float32
BF16 = jnp.bfloat16
NT = (((1,), (1,)), ((), ()))
TN = (((0,), (0,)), ((), ()))


SMALL = pltpu.CompilerParams(vmem_limit_bytes=16 * 2**20)


def vmem_spec():
    return pl.BlockSpec(memory_space=pltpu.VMEM)


def cost(flops, moved):
    return pl.CostEstimate(flops=flops, bytes_accessed=moved, transcendentals=0)


def is_first_core():
    return lax.rem(lax.axis_index(CTX), 2) == 0


def hbm_spec():
    return pl.BlockSpec(memory_space=pltpu.HBM)


def run_copies(pairs, sems):
    copies = [pltpu.make_async_copy(source, target, sems.at[i]) for i, (source, target) in enumerate(pairs)]
    for copy in copies:
        copy.start()
    return copies


def halves_kernel(*refs):
    x_ref, z_ref, b_ref, c_ref, dt_ref, k_ref, v_ref, q_ref, bias_ref, alog_ref, skip_ref = refs[:11]
    mine_ref, theirs_ref, kv_ref, even_ref, odd_ref, small, sems = refs[11:]
    half = x_ref.shape[1] // 2
    tiles = half // 128
    heads = bias_ref.shape[0] // 2
    first = is_first_core()
    pairs = [(ref, small.at[i]) for i, ref in enumerate((bias_ref, alog_ref, skip_ref))]
    pairs += [(k_ref, kv_ref.at[:TOK]), (v_ref, kv_ref.at[TOK:])]
    for out_ref, low in ((theirs_ref, jnp.logical_not(first)), (mine_ref, first)):
        base = jnp.where(low, 0, half)
        for which, ref in enumerate((x_ref, z_ref)):
            for t in range(tiles):
                row = (which * tiles + t) * TOK
                columns = pl.ds(pl.multiple_of(base + t * 128, 128), 128)
                pairs.append((ref.at[:, columns], out_ref.at[row : row + TOK]))
        row = 2 * tiles * TOK
        pairs.append((b_ref, out_ref.at[row : row + TOK]))
        pairs.append((c_ref, out_ref.at[row + TOK : row + 2 * TOK]))
        pairs.append((dt_ref, out_ref.at[row + 2 * TOK : row + 2 * TOK + 2 * heads]))
    for out_ref, low in ((even_ref, first), (odd_ref, jnp.logical_not(first))):
        start = pl.multiple_of(jnp.where(low, 0, HALF), HALF)
        pairs.append((q_ref.at[pl.ds(start, HALF), :], out_ref))
    copies = run_copies(pairs, sems)
    for copy in copies[:3]:
        copy.wait()
    head_row = lax.broadcasted_iota(jnp.int32, (heads, TOK), 0)
    at = jnp.where(first, 0, heads)
    bias, rate, skip = [jnp.zeros((heads, TOK), F32)] * 3
    for h in range(heads):
        bias = jnp.where(head_row == h, small[0, at + h], bias)
        rate = jnp.where(head_row == h, small[1, at + h], rate)
        skip = jnp.where(head_row == h, small[2, at + h], skip)
    rate = jnp.exp(rate)
    rest = jnp.concatenate([bias, bias, rate, rate, skip, skip], axis=0)
    start = row + 2 * TOK + 2 * heads
    for part in range(3):
        rounded = rest.astype(BF16)
        mine_ref[start + part * 6 * heads : start + (part + 1) * 6 * heads, :] = rounded
        rest = rest - rounded.astype(F32)
    for copy in copies[3:]:
        copy.wait()


def halves(m_x, m_z, m_b, m_c, dt_turned, keys, values, query, dt_bias, a_log, d_skip):
    heads = dt_bias.shape[0] // 2
    rows = (m_x.shape[1] // 128 + 2) * TOK + 2 * heads
    tiles = m_x.shape[1] // 256
    half_query = jax.ShapeDtypeStruct((HALF, query.shape[1]), BF16)
    return pl.pallas_call(
        halves_kernel,
        out_shape=(
            jax.ShapeDtypeStruct((rows + 18 * heads, TOK), BF16),
            jax.ShapeDtypeStruct((rows, TOK), BF16),
            jax.ShapeDtypeStruct((2 * TOK, HEAD_SIZE), BF16),
            half_query,
            half_query,
        ),
        in_specs=[hbm_spec()] * 11,
        out_specs=(vmem_spec(),) * 5,
        scratch_shapes=[
            pltpu.SMEM((3, 2 * heads), F32),
            pltpu.SemaphoreType.DMA((5 + 2 * (2 * tiles + 3) + 2,)),
        ],
        cost_estimate=cost(10**6, 8 * rows * TOK),
        name="halves",
    )(m_x, m_z, m_b, m_c, dt_turned, keys, values, query, dt_bias, a_log, d_skip)


def pair_of(mine_ref, got_ref, first, row):
    mine, got = mine_ref[row : row + TOK, :], got_ref[row : row + TOK, :]
    one, two = jnp.where(first, mine, got), jnp.where(first, got, mine)
    return (
        jnp.concatenate([one[:HALF], two[:HALF]], axis=0),
        jnp.concatenate([two[HALF:], one[HALF:]], axis=0),
    )


def softplus(v):
    return jnp.maximum(v, 0.0) + jnp.log1p(jnp.exp(-jnp.abs(v)))


def local_kernel(mine_ref, got_ref, states_ref, inner_ref, grown_ref):
    heads = (mine_ref.shape[0] - got_ref.shape[0]) // 18
    tiles = heads * MP // 128
    first = is_first_core()
    row = 2 * tiles * TOK
    b_runs = pair_of(mine_ref, got_ref, first, row)
    c_runs = pair_of(mine_ref, got_ref, first, row + TOK)

    lane = lax.broadcasted_iota(jnp.int32, (heads, TOK), 1)
    low = lane < HALF
    dt_rows = slice(row + 2 * TOK, row + 2 * TOK + 2 * heads)
    mine_dt, got_dt = mine_ref[dt_rows, :].astype(F32), got_ref[dt_rows, :].astype(F32)
    coef = sum(
        mine_ref[dt_rows.stop + part * 6 * heads : dt_rows.stop + (part + 1) * 6 * heads, :].astype(F32) for part in range(3)
    )
    mine_dt = jnp.where(first, mine_dt[:heads], mine_dt[heads:])
    got_dt = jnp.where(first, got_dt[:heads], got_dt[heads:])
    one, two = jnp.where(first, mine_dt, got_dt), jnp.where(first, got_dt, mine_dt)
    two = pltpu.roll(two, HALF, 1)
    raw = jnp.concatenate([jnp.where(low, one, two), jnp.where(low, two, one)], axis=0)
    bias, rate = coef[: 2 * heads, :], coef[2 * heads : 4 * heads, :]
    dt = softplus(raw + bias)
    run = -dt * rate
    lanes = lax.broadcasted_iota(jnp.int32, (2 * heads, TOK), 1)
    shift = 1
    while shift < TOK:
        run = run + jnp.where(lanes >= shift, pltpu.roll(run, shift, 1), 0.0)
        shift *= 2
    last = jnp.broadcast_to(run[:, TOK - 1 :], run.shape)
    tail = jnp.exp(last - run) * dt
    columns = jnp.concatenate([run, tail, jnp.zeros((TOK - 4 * heads, TOK), F32)], axis=0).T
    grown_ref[...] = jnp.exp(columns[:, : 2 * heads])
    high = last.astype(BF16)
    middle = (last - high.astype(F32)).astype(BF16)
    least = (last - high.astype(F32) - middle.astype(F32)).astype(BF16)
    parts = [part.astype(F32) for part in (high, middle, least)]

    row_id = lax.broadcasted_iota(jnp.int32, (TOK, TOK), 0)
    col_id = lax.broadcasted_iota(jnp.int32, (TOK, TOK), 1)
    seen = row_id >= col_id
    left = col_id < MP
    crosses = [lax.dot_general(c_runs[q], b_runs[q], NT, preferred_element_type=F32) for q in range(2)]
    for t in range(tiles):
        x_runs = pair_of(mine_ref, got_ref, first, t * TOK)
        for q in range(2):
            at = q * heads + 2 * t
            x = x_runs[q]
            wide = x.astype(F32)
            weights = []
            for e in range(2):
                spread = columns[:, at + e : at + e + 1] - run[at + e : at + e + 1, :]
                decay = jnp.exp(jnp.where(seen, spread, -jnp.inf))
                weights.append((crosses[q] * decay * dt[at + e : at + e + 1, :]).astype(BF16))
            both = jnp.dot(jnp.concatenate(weights, axis=0), x, preferred_element_type=F32)
            skip_row = 4 * heads + 2 * t
            skip = jnp.where(left, coef[skip_row : skip_row + 1, :], coef[skip_row + 1 : skip_row + 2, :])
            inner_ref[q, t] = jnp.where(left, both[:TOK], both[TOK:]) + skip * wide
            offset = 2 * heads + at
            tails = jnp.where(left, columns[:, offset : offset + 1], columns[:, offset + 1 : offset + 2])
            state = lax.dot_general((wide * tails).astype(BF16), b_runs[q], TN, preferred_element_type=F32)
            state = state.astype(BF16)
            for piece in range(4):
                states_ref[4 * t + piece, q * 32 : q * 32 + 32, :] = state[piece * 32 : piece * 32 + 32, :]
    part_row = lax.broadcasted_iota(jnp.int32, (8, TOK), 0)
    for h in range(heads):
        block = jnp.zeros((8, TOK), F32)
        for q in range(2):
            at = q * heads + h
            for i in range(3):
                block = jnp.where(part_row == 3 * q + i, parts[i][at : at + 1, :], block)
        for piece in range(2):
            states_ref[2 * h + piece, 64:72, :] = block.astype(BF16)


def local_states(mine, got):
    heads = (mine.shape[0] - got.shape[0]) // 18
    width = heads * MP
    return pl.pallas_call(
        local_kernel,
        out_shape=(
            jax.ShapeDtypeStruct((width // 32, 72, MN), BF16),
            jax.ShapeDtypeStruct((2, width // 128, TOK, 128), F32),
            jax.ShapeDtypeStruct((TOK, 2 * heads), F32),
        ),
        in_specs=[vmem_spec()] * 2,
        out_specs=(vmem_spec(), vmem_spec(), vmem_spec()),
        compiler_params=SMALL,
        cost_estimate=cost(10**9, 10**6),
        name="local",
    )(mine, got)


def chain_kernel(states_ref, out_ref):
    count = states_ref.shape[0]
    state = jnp.zeros((32, MN), F32)
    for q in range(2):
        for k in range(count) if q == 0 else reversed(range(count)):
            out_ref[k, q * 32 : q * 32 + 32, :] = state.astype(BF16)
            parts = states_ref[k, 64:72, :].astype(F32)
            decay = jnp.exp(parts[3 * q : 3 * q + 1] + parts[3 * q + 1 : 3 * q + 2] + parts[3 * q + 2 : 3 * q + 3])
            state = state * decay + states_ref[k, q * 32 : q * 32 + 32, :].astype(F32)


def chain(states):
    count = states.shape[0]
    return pl.pallas_call(
        chain_kernel,
        out_shape=jax.ShapeDtypeStruct((count, 64, MN), BF16),
        in_specs=[vmem_spec()],
        out_specs=vmem_spec(),
        compiler_params=SMALL,
        cost_estimate=cost(10**6, 10**6),
        name="chain",
    )(states)


def gate_kernel(entering_ref, inner_ref, grown_ref, mine_ref, got_ref, even_ref, odd_ref):
    tiles = inner_ref.shape[1]
    heads = 2 * tiles
    first = is_first_core()
    c_runs = pair_of(mine_ref, got_ref, first, (2 * tiles + 1) * TOK)
    left = lax.broadcasted_iota(jnp.int32, (TOK, 128), 1) < MP
    for t in range(tiles):
        z_runs = pair_of(mine_ref, got_ref, first, (tiles + t) * TOK)
        results = []
        for q in range(2):
            at = q * heads + 2 * t
            state = entering_ref[4 * t : 4 * t + 4, q * 32 : q * 32 + 32, :].reshape(128, MN)
            carried = lax.dot_general(c_runs[q], state, NT, preferred_element_type=F32)
            grown = jnp.where(left, grown_ref[:, at : at + 1], grown_ref[:, at + 1 : at + 2])
            y = inner_ref[q, t] + carried * grown
            z = z_runs[q].astype(F32)
            results.append((y * (z / (1.0 + jnp.exp(-z)))).astype(BF16))
        even_ref[:, t * 128 : t * 128 + 128] = jnp.where(first, results[0], results[1])
        odd_ref[:, t * 128 : t * 128 + 128] = jnp.where(first, results[1], results[0])


def gate(entering, inner, grown, mine, got):
    shape = jax.ShapeDtypeStruct((TOK, inner.shape[1] * 128), BF16)
    return pl.pallas_call(
        gate_kernel,
        out_shape=(shape, shape),
        in_specs=[vmem_spec()] * 5,
        out_specs=(vmem_spec(), vmem_spec()),
        compiler_params=SMALL,
        cost_estimate=cost(10**8, 10**6),
        name="gate",
    )(entering, inner, grown, mine, got)


def norm_kernel(half_count, even_ref, odd_ref, even_far_ref, odd_far_ref, gain_ref, out_ref):
    early = lax.axis_index(CTX) < half_count
    width = even_ref.shape[1]
    even, odd = even_ref[...] + even_far_ref[...], odd_ref[...] + odd_far_ref[...]
    one = jnp.where(early, even, odd).astype(F32)
    two = jnp.where(early, odd, even).astype(F32)
    power = jnp.sum(one * one + two * two, axis=1, keepdims=True) * (0.5 / width)
    scale = lax.rsqrt(power + norm_eps)
    out_ref[:, :width] = ((one * scale) * gain_ref[:, :width]).astype(BF16)
    out_ref[:, width:] = ((two * scale) * gain_ref[:, width:]).astype(BF16)


def gated_norm(even, odd, even_far, odd_far, gain, half_count):
    return pl.pallas_call(
        functools.partial(norm_kernel, half_count),
        out_shape=jax.ShapeDtypeStruct((TOK, 2 * even.shape[1]), BF16),
        in_specs=[vmem_spec()] * 5,
        out_specs=vmem_spec(),
        compiler_params=SMALL,
        cost_estimate=cost(10**6, 10**6),
        name="norm",
    )(even, odd, even_far, odd_far, gain.reshape(1, -1))


def attend_kernel(count, q0_ref, q1_ref, kv, out_ref, q_s, m_s, l_s, acc_s):
    blocks = 8
    me = lax.axis_index(CTX)
    keys_here = blocks * HALF
    full = (me * TOK) // keys_here
    heads = q0_ref.shape[1] // HEAD_SIZE
    for h in range(heads):
        columns = slice(h * HEAD_SIZE, (h + 1) * HEAD_SIZE)
        q_s[h * TOK : h * TOK + HALF, :] = q0_ref[:, columns]
        q_s[h * TOK + HALF : (h + 1) * TOK, :] = q1_ref[:, columns]
    m_s[...] = jnp.full(m_s.shape, -1e30, F32)
    l_s[...] = jnp.zeros(l_s.shape, F32)
    acc_s[...] = jnp.zeros(acc_s.shape, F32)
    scale = math.log2(math.e) / math.sqrt(HEAD_SIZE)
    rows = heads * TOK

    def step(first_block, block_count, diagonal):
        def piece(offset):
            parts = []
            for p in range(block_count):
                c = first_block + p
                early = c < count
                source = jnp.where(early, c, 2 * count - 1 - c)
                start = pl.multiple_of(jnp.where(early, 0, HALF) + offset, HALF)
                parts.append(kv[source, pl.ds(start, HALF), :])
            return jnp.concatenate(parts, axis=0)

        k_rows, v_rows = piece(0), piece(TOK)
        scores = lax.dot_general(k_rows, q_s[...], NT, preferred_element_type=F32)
        if diagonal:
            key = lax.broadcasted_iota(jnp.int32, (TOK, rows), 0)
            column = lax.broadcasted_iota(jnp.int32, (TOK, rows), 1)
            seen = key <= jnp.bitwise_and(column, TOK - 1)
            scores = jnp.where(seen, scores, -1e30)
        old = m_s[...]
        new = jnp.maximum(old, jnp.max(scores, axis=0, keepdims=True))
        expons = jnp.exp2((scores - new) * scale)
        if diagonal:
            expons = jnp.where(seen, expons, 0.0)
        factor = jnp.exp2((old - new) * scale)
        m_s[...] = new
        l_s[...] = l_s[...] * factor + jnp.sum(expons, axis=0, keepdims=True)
        acc_s[...] = acc_s[...] * factor + lax.dot_general(
            v_rows, expons.astype(BF16), TN, preferred_element_type=F32
        )

    lax.fori_loop(0, full, lambda index, _: step(index * blocks, blocks, False), None)
    left = lax.rem(me * TOK, keys_here) // TOK
    for whole in range(1, keys_here // TOK):

        @pl.when(left == whole)
        def _():
            step(full * blocks, 2 * whole, False)

    step(2 * me, 2, True)
    result = acc_s[...] / l_s[...]
    for h in range(heads):
        columns = slice(h * TOK, (h + 1) * TOK)
        out_ref[:, h * HEAD_SIZE : (h + 1) * HEAD_SIZE] = result[:, columns].T.astype(BF16)


def attend(q0, q1, gathered):
    count, rows, _ = gathered.shape
    heads = q0.shape[1] // HEAD_SIZE
    return pl.pallas_call(
        functools.partial(attend_kernel, count),
        out_shape=jax.ShapeDtypeStruct((TOK, q0.shape[1]), BF16),
        in_specs=[vmem_spec()] * 3,
        out_specs=vmem_spec(),
        scratch_shapes=[
            pltpu.VMEM((heads * TOK, HEAD_SIZE), BF16),
            pltpu.VMEM((1, heads * TOK), F32),
            pltpu.VMEM((1, heads * TOK), F32),
            pltpu.VMEM((HEAD_SIZE, heads * TOK), F32),
        ],
        compiler_params=SMALL,
        cost_estimate=cost(4 * heads * TOK * count * TOK * HEAD_SIZE, count * rows * TOK),
        name="attend",
    )(q0, q1, gathered)


def permute(value, target, sources):
    return lax.ppermute(value, CTX, [(d, target(d)) for d in sources])


RELAY_HOPS = 8
RESULT_RELAYS = 1


def relay(value, count, chips):
    sources = range(count - 2 * chips, count)
    return permute(value, lambda d: (d + 2 * RELAY_HOPS) % count, sources)


def forward(value, count, chips, target):
    sources = range(count - 2 * chips, count)
    return lax.ppermute(value, CTX, [((d + 2 * RELAY_HOPS) % count, target(d)) for d in sources])


def layer(query, keys, values, m_x, m_z, m_b, m_c, dt_raw, dt_bias, a_log, d_skip, norm_gain):
    count = lax.axis_size(CTX)
    chips = count // 2
    mine, theirs, pairs, *pieces = halves(
        m_x, m_z, m_b, m_c, dt_raw.T, keys, values, query, dt_bias, a_log, d_skip
    )
    gathered = lax.all_gather(pairs, CTX)
    got = permute(theirs, lambda d: d ^ 1, range(count))
    states, inner, grown = local_states(mine, got)
    same_core = [list(range(core, count, 2)) for core in range(2)]
    exchange = functools.partial(
        lax.all_to_all, axis_name=CTX, split_axis=0, concat_axis=0, tiled=True, axis_index_groups=same_core
    )
    block = [lambda d: d if d % 2 == 0 else 2 * count - 1 - d, lambda d: 2 * count - 1 - d if d % 2 == 0 else d]
    queries = []
    for slot in range(2):
        queries.append(permute(pieces[slot], lambda d: block[slot](d) // 2, range(count)))
    exchanged = exchange(states)
    entering = exchange(chain(exchanged))

    even, odd = gate(entering, inner, grown, mine, got)
    goals = [
        lambda d: d // 2 if d % 2 == 0 else count - 1 - d // 2,
        lambda d: count - 1 - d // 2 if d % 2 == 0 else d // 2,
    ]
    results = (even, odd)
    direct = [permute(results[slot], goals[slot], range(count - 2 * RESULT_RELAYS)) for slot in range(2)]
    relayed = [relay(results[slot], count, RESULT_RELAYS) for slot in range(2)]
    ahead = [forward(relayed[slot], count, RESULT_RELAYS, goals[slot]) for slot in range(2)]
    context = attend(queries[0], queries[1], gathered)
    direct, ahead, context = lax.optimization_barrier((direct, ahead, context))
    mixed = gated_norm(*direct, *ahead, norm_gain, chips)
    return (context, mixed)


def solution(mesh):
    rows, heads = P(GRP_CTX, "hd"), P("hd")
    return jax.shard_map(
        layer,
        mesh=mesh,
        in_specs=(rows,) * 8 + (heads,) * 4,
        out_specs=(rows, rows),
        check_vma=False,
    )
```
